16 devices in a mesh: dp: 4 (over z, y), ep: 4 (over x, core).
Axes of the slice: x: 2, y: 2, z: 2, core: 2. Of those that a mesh axis runs over, the one named last changes fastest.
Arguments:
- hidden: bfloat16 [16384, 2048], P(('dp', 'ep')), parts along dimension 0
- expert_ids: int32 [16384, 2], P(('dp', 'ep')), parts along dimension 0
- norm_gain: bfloat16 [2048], replicated
- w_router: bfloat16 [2048, 8], replicated
- w_gate: bfloat16 [8, 2048, 5632], P('ep')
- w_up: bfloat16 [8, 2048, 5632], P('ep')
- w_down: bfloat16 [8, 5632, 2048], P('ep')
Outputs:
- output: bfloat16 [16384, 2048], P(('dp', 'ep')), parts along dimension 0
There are 4 independent parts. The reference program is written for one: setup_inputs(seed, part) draws one part's arguments, and reference() takes and returns one part's arrays. A program takes and returns all parts, laid end to end along the dimension named above; an argument that names none is the same for every part.
All inputs are finite; a program needn't handle non-finite values.
Results may differ from the reference program's by a relative error of at most 0.00119.
Values are sent between devices in bfloat16 or wider.
A program may use at most 1 GiB of HBM per device.

```python
import jax
import jax.numpy as jnp
from jax import lax

D = 2048
FF = 5632
EXPERTS = 8
TOK = 1024
GROUP = 4
NORM_EPS = 1e-5
TOKENS = TOK * GROUP
CAPACITY = (5 * TOK + 2 * EXPERTS - 1) // (2 * EXPERTS)


def draw_expert_ids(key):
    k_hot, k_ticket, k_cover, k_offset = jax.random.split(key, 4)
    hot_expert = jax.random.randint(k_hot, (GROUP, 1), 0, EXPERTS)
    ticket = jax.random.randint(k_ticket, (GROUP, TOK), 0, EXPERTS + 3)
    first_pick = jnp.where(ticket < EXPERTS, ticket, hot_expert)
    token_pos = jnp.arange(TOK)[None, :]
    cover_shift = jax.random.randint(k_cover, (GROUP, 1), 0, EXPERTS)
    first_pick = jnp.where(token_pos < EXPERTS, (token_pos + cover_shift) % EXPERTS, first_pick)
    offset = jax.random.randint(k_offset, (GROUP, TOK), 1, EXPERTS)
    second_pick = (first_pick + offset) % EXPERTS
    return jnp.stack([first_pick, second_pick], axis=-1).reshape(TOKENS, 2).astype(jnp.int32)


def setup_inputs(seed: int = 0, part: int = 0) -> dict:
    key = jax.random.key(seed)
    k_hidden, k_ids, k_gain, k_router, k_gate, k_up, k_down = jax.random.split(key, 7)
    k_hidden = jax.random.fold_in(k_hidden, part)
    k_ids = jax.random.fold_in(k_ids, part)
    hidden = jax.random.normal(k_hidden, (TOKENS, D), jnp.float32).astype(jnp.bfloat16)
    expert_ids = draw_expert_ids(k_ids)
    norm_gain = (1.0 + 0.3 * jax.random.normal(k_gain, (D,), jnp.float32)).astype(jnp.bfloat16)
    w_router = (2.0 * D ** -0.5 * jax.random.normal(k_router, (D, EXPERTS), jnp.float32)).astype(jnp.bfloat16)
    w_gate = (D ** -0.5 * jax.random.normal(k_gate, (EXPERTS, D, FF), jnp.float32)).astype(jnp.bfloat16)
    w_up = (D ** -0.5 * jax.random.normal(k_up, (EXPERTS, D, FF), jnp.float32)).astype(jnp.bfloat16)
    w_down = (2.0 * FF ** -0.5 * jax.random.normal(k_down, (EXPERTS, FF, D), jnp.float32)).astype(jnp.bfloat16)
    return {"hidden": hidden, "expert_ids": expert_ids, "norm_gain": norm_gain, "w_router": w_router, "w_gate": w_gate, "w_up": w_up, "w_down": w_down}


def rms_norm(hidden, norm_gain):
    hidden_f32 = hidden.astype(jnp.float32)
    mean_sq = jnp.mean(hidden_f32 * hidden_f32, axis=-1, keepdims=True)
    return (hidden_f32 * lax.rsqrt(mean_sq + NORM_EPS) * norm_gain.astype(jnp.float32)).astype(jnp.bfloat16)


def slot_positions(shard_ids):
    slot_order = jnp.concatenate([shard_ids[:, 0], shard_ids[:, 1]])
    hit_table = (slot_order[:, None] == jnp.arange(EXPERTS)[None, :]).astype(jnp.int32)
    seen_before = jnp.cumsum(hit_table, axis=0) - hit_table
    slot_rank = jnp.sum(seen_before * hit_table, axis=1)
    return slot_rank.reshape(2, TOK).T


def expert_ffn(operands):
    rows, gate_w, up_w, down_w = operands
    gate_proj = jnp.dot(rows, gate_w, preferred_element_type=jnp.float32)
    up_proj = jnp.dot(rows, up_w, preferred_element_type=jnp.float32)
    hidden_act = (jax.nn.silu(gate_proj) * up_proj).astype(jnp.bfloat16)
    return jnp.dot(hidden_act, down_w, preferred_element_type=jnp.float32).astype(jnp.bfloat16)


def reference(hidden, expert_ids, norm_gain, w_router, w_gate, w_up, w_down):
    normed = rms_norm(hidden, norm_gain)
    logits = jnp.dot(normed, w_router, preferred_element_type=jnp.float32)
    picked = jnp.take_along_axis(logits, expert_ids, axis=1)
    gate_probs = jax.nn.softmax(picked, axis=-1)
    positions = jax.vmap(slot_positions)(expert_ids.reshape(GROUP, TOK, 2)).reshape(TOKENS, 2)
    source = (jnp.arange(TOKENS) // TOK)[:, None]
    kept = positions < CAPACITY
    buffer_row = jnp.where(kept, source * CAPACITY + positions, GROUP * CAPACITY)
    rows_in = jnp.broadcast_to(normed[:, None, :], (TOKENS, 2, D))
    buffers = jnp.zeros((EXPERTS, GROUP * CAPACITY, D), jnp.bfloat16)
    buffers = buffers.at[expert_ids, buffer_row].set(rows_in, mode="drop")
    expert_out = lax.map(expert_ffn, (buffers, w_gate, w_up, w_down))
    fetched = expert_out[expert_ids, jnp.minimum(buffer_row, GROUP * CAPACITY - 1)]
    fetched = jnp.where(kept[:, :, None], fetched.astype(jnp.float32), 0.0)
    mixed_sum = jnp.sum(gate_probs[:, :, None] * fetched, axis=1)
    return (hidden.astype(jnp.float32) + mixed_sum).astype(jnp.bfloat16)
```

```python
import functools

import jax
import jax.numpy as jnp
from jax import lax
from jax.experimental import pallas as pl
from jax.experimental.pallas import tpu as pltpu
from jax.sharding import PartitionSpec as P


NORM_EPS = 1e-5
LANES = 256
F_TILE = 512
SLOTS = 3
VMEM_LIMIT = 60 * 1024 * 1024
ANY = pl.BlockSpec(memory_space=pltpu.HBM)
SMEM = pl.BlockSpec(memory_space=pltpu.SMEM)


def norm_kernel(hidden_ref, gain_ref, out_ref):
    hidden_f32 = hidden_ref[...].astype(jnp.float32)
    mean_sq = jnp.mean(hidden_f32 * hidden_f32, axis=-1, keepdims=True)
    out_ref[...] = (hidden_f32 * lax.rsqrt(mean_sq + NORM_EPS) * gain_ref[...].astype(jnp.float32)).astype(jnp.bfloat16)


def rms_norm(hidden, norm_gain):
    rows, width = hidden.shape
    tile = 256
    return pl.pallas_call(
        norm_kernel,
        grid=(rows // tile,),
        in_specs=[pl.BlockSpec((tile, width), lambda i: (i, 0)), pl.BlockSpec((1, width), lambda i: (0, 0))],
        out_specs=pl.BlockSpec((tile, width), lambda i: (i, 0)),
        out_shape=jax.ShapeDtypeStruct((rows, width), jnp.bfloat16),
        cost_estimate=pl.CostEstimate(flops=8 * rows * width, bytes_accessed=4 * rows * width, transcendentals=rows),
        name="norm",
    )(hidden, norm_gain.reshape(1, width))


def ffn_kernel(experts, blocks, pick, variants, capacity, n_src, scal_ref, pos_ref, *refs):
    srcs = refs[:n_src]
    wg_ref, wu_ref, wd_ref, _ = refs[n_src:n_src + 4]
    outs = refs[n_src + 4:n_src + 4 + blocks]
    token_ref = refs[n_src + 4 + blocks]
    ubuf, x_buf, act, obuf, gbuf, ubuf_w, dbuf, usem, gsem, dsem, osem = refs[n_src + 5 + blocks:]
    width, ff = wg_ref.shape[1], wg_ref.shape[2]
    n_up, n_down = ff // F_TILE, width // LANES

    def up_copies(expert, tile, slot):
        cols = pl.ds(pl.multiple_of(tile * F_TILE, F_TILE), F_TILE)
        return (pltpu.make_async_copy(wg_ref.at[expert, :, cols], gbuf.at[slot], gsem.at[0, slot]),
                pltpu.make_async_copy(wu_ref.at[expert, :, cols], ubuf_w.at[slot], gsem.at[1, slot]))

    def down_copy(expert, tile, slot):
        cols = pl.ds(pl.multiple_of(tile * LANES, LANES), LANES)
        return pltpu.make_async_copy(wd_ref.at[expert, :, cols], dbuf.at[slot], dsem.at[slot])

    if pick:
        for core in range(2):
            @pl.when(scal_ref[0] == core)
            def _():
                pltpu.make_async_copy(srcs[core], ubuf.at[0], usem.at[0]).start()
    else:
        for b in range(blocks):
            pltpu.make_async_copy(srcs[b], ubuf.at[b], usem.at[b]).start()
    for tile in range(SLOTS - 1):
        for copy in up_copies(experts[0], tile, tile):
            copy.start()

    token_ref[...] = jnp.zeros_like(token_ref)
    obuf[...] = jnp.zeros_like(obuf)
    for b in range(blocks):
        pltpu.make_async_copy(srcs[b], ubuf.at[b], usem.at[b]).wait()

    def counts_of(k):
        first = scal_ref[1 + k * blocks]
        start = (first + 15) // 16 * 16
        if blocks == 1:
            return 0, first
        return start, start + scal_ref[2 + k * blocks]

    def out_copies(k, start):
        offsets = [0] if blocks == 1 else [0, pl.multiple_of(start, 16)]
        return [pltpu.make_async_copy(obuf.at[k, pl.ds(offset, capacity), :], outs[b].at[pl.ds(k * capacity, capacity), :],
                                      osem.at[k * blocks + b]) for b, offset in enumerate(offsets)]

    rows_iota = lax.broadcasted_iota(jnp.int32, (capacity, ubuf.shape[1]), 0)
    for k in range(len(experts)):
        start, _ = counts_of(k)
        for b in range(blocks):
            pos = pos_ref[pl.ds(k * blocks + b, 1), :]
            onehot = jnp.where(rows_iota == pos, 1.0, 0.0).astype(jnp.bfloat16)
            offset = 0 if b == 0 else pl.multiple_of(start, 16)

            @pl.loop(0, width // F_TILE)
            def _(n, onehot=onehot, b=b, offset=offset, k=k):
                cols = pl.ds(pl.multiple_of(n * F_TILE, F_TILE), F_TILE)
                picked = jnp.dot(onehot, ubuf[b, :, cols], preferred_element_type=jnp.float32)
                x_buf[k, pl.ds(offset, capacity), cols] = picked.astype(jnp.bfloat16)

    for k, expert in enumerate(experts):
        start, total = counts_of(k)
        last = k == len(experts) - 1

        def run(rows, k=k, expert=expert, last=last):
            base_up = (k * n_up) % SLOTS
            base_down = (k * n_down) % SLOTS

            @pl.loop(0, n_up)
            def _(i):
                ahead = i + SLOTS - 1

                @pl.when(ahead < n_up)
                def _():
                    for copy in up_copies(expert, ahead, lax.rem(ahead + base_up, SLOTS)):
                        copy.start()

                @pl.when(ahead >= n_up)
                def _():
                    down_copy(expert, ahead - n_up, lax.rem(ahead - n_up + base_down, SLOTS)).start()

                slot = lax.rem(i + base_up, SLOTS)
                for copy in up_copies(expert, i, slot):
                    copy.wait()
                for half in range(F_TILE // LANES):
                    cols = slice(half * LANES, (half + 1) * LANES)
                    gate = jnp.dot(x_buf[k, :rows, :], gbuf[slot, :, cols], preferred_element_type=jnp.float32)
                    up = jnp.dot(x_buf[k, :rows, :], ubuf_w[slot, :, cols], preferred_element_type=jnp.float32)
                    at = pl.ds(pl.multiple_of(i * F_TILE + half * LANES, LANES), LANES)
                    act[:rows, at] = (jax.nn.silu(gate) * up).astype(jnp.bfloat16)

            @pl.loop(0, n_down)
            def _(n):
                ahead = n + SLOTS - 1

                @pl.when(ahead < n_down)
                def _():
                    down_copy(expert, ahead, lax.rem(ahead + base_down, SLOTS)).start()

                if not last:
                    @pl.when(ahead >= n_down)
                    def _():
                        tile = ahead - n_down
                        for copy in up_copies(experts[k + 1], tile, lax.rem(tile + (k + 1) * n_up, SLOTS)):
                            copy.start()

                slot = lax.rem(n + base_down, SLOTS)
                down_copy(expert, n, slot).wait()
                out = jnp.dot(act[:rows, :], dbuf[slot], preferred_element_type=jnp.float32)
                obuf[k, :rows, pl.ds(pl.multiple_of(n * LANES, LANES), LANES)] = out.astype(jnp.bfloat16)

        low = 0
        for v in variants:
            hit = total <= v if v == variants[0] else ((total > low) & (total <= v))
            pl.when(hit)(functools.partial(run, v))
            low = v
        for copy in out_copies(k, start):
            copy.start()
    for k in range(len(experts)):
        for copy in out_copies(k, counts_of(k)[0]):
            copy.wait()


def ffn_pass(experts, blocks, pick, variants, capacity, scal, pos, srcs, w_gate, w_up, w_down, order):
    tok_rows, width = srcs[0].shape
    ff = w_gate.shape[2]
    n_out = len(experts) * blocks
    most = capacity * blocks
    bf16 = jnp.bfloat16
    rows = n_out * capacity
    outs = pl.pallas_call(
        functools.partial(ffn_kernel, experts, blocks, pick, variants, capacity, len(srcs)),
        in_specs=[SMEM, pl.BlockSpec(memory_space=pltpu.VMEM)] + [ANY] * (len(srcs) + 4),
        out_specs=[ANY] * blocks + [pl.BlockSpec(memory_space=pltpu.VMEM)],
        out_shape=[jax.ShapeDtypeStruct((len(experts) * capacity, width), bf16)] * blocks + [jax.ShapeDtypeStruct((8, 128), jnp.int32)],
        scratch_shapes=[
            pltpu.VMEM((blocks, tok_rows, width), bf16),
            pltpu.VMEM((len(experts), most, width), bf16),
            pltpu.VMEM((most, ff), bf16),
            pltpu.VMEM((len(experts), most, width), bf16),
            pltpu.VMEM((SLOTS, width, F_TILE), bf16),
            pltpu.VMEM((SLOTS, width, F_TILE), bf16),
            pltpu.VMEM((SLOTS, ff, LANES), bf16),
            pltpu.SemaphoreType.DMA((2,)),
            pltpu.SemaphoreType.DMA((2, SLOTS)),
            pltpu.SemaphoreType.DMA((SLOTS,)),
            pltpu.SemaphoreType.DMA((n_out,)),
        ],
        compiler_params=pltpu.CompilerParams(vmem_limit_bytes=VMEM_LIMIT),
        cost_estimate=pl.CostEstimate(flops=6 * rows * width * ff, bytes_accessed=6 * len(experts) * width * ff, transcendentals=rows * ff),
    )(scal, pos, *srcs, w_gate, w_up, w_down, order)
    return outs[:blocks], outs[blocks]


def combine_kernel(n_buf, pick, last, scal_ref, idx0_ref, idx1_ref, p0_ref, p1_ref, *refs):
    bufs = refs[:n_buf]
    rest = refs[n_buf:]
    held, sem = rest[-2:]
    out_ref = rest[-3]
    used = sem.shape[0]
    each = held.shape[0] // used

    @pl.when(pl.program_id(0) == 0)
    def _():
        if pick:
            for core in range(2):
                @pl.when(scal_ref[0] == core)
                def _():
                    for b in range(used):
                        pltpu.make_async_copy(bufs[core * used + b], held.at[pl.ds(b * each, each), :], sem.at[b]).start()
        else:
            for b in range(used):
                pltpu.make_async_copy(bufs[b], held.at[pl.ds(b * each, each), :], sem.at[b]).start()
        for b in range(used):
            pltpu.make_async_copy(bufs[b], held.at[pl.ds(b * each, each), :], sem.at[b]).wait()

    lanes = lax.broadcasted_iota(jnp.int32, (idx0_ref.shape[0], held.shape[0]), 1)
    hot0 = jnp.where(lanes == idx0_ref[...], 1.0, 0.0).astype(jnp.bfloat16)
    hot1 = jnp.where(lanes == idx1_ref[...], 1.0, 0.0).astype(jnp.bfloat16)
    for n in range(held.shape[1] // F_TILE):
        cols = slice(n * F_TILE, (n + 1) * F_TILE)
        mixed = p0_ref[...] * jnp.dot(hot0, held[:, cols], preferred_element_type=jnp.float32)
        mixed += p1_ref[...] * jnp.dot(hot1, held[:, cols], preferred_element_type=jnp.float32)
        if last:
            hidden_ref, part_ref = rest[0], rest[1]
            out_ref[:, cols] = (hidden_ref[:, cols].astype(jnp.float32) + (part_ref[:, cols] + mixed)).astype(jnp.bfloat16)
        else:
            out_ref[:, cols] = mixed


def combine(scal, idx, probs, bufs, pick, extra, order):
    tok_rows = idx[0].shape[0]
    capacity, width = bufs[0].shape
    used = len(bufs) // 2 if pick else len(bufs)
    tile = 256
    last = bool(extra)
    column = pl.BlockSpec((tile, 1), lambda i: (i, 0))
    block = pl.BlockSpec((tile, width), lambda i: (i, 0))
    return pl.pallas_call(
        functools.partial(combine_kernel, len(bufs), pick, last),
        grid=(tok_rows // tile,),
        in_specs=[SMEM] + [column] * 4 + [ANY] * len(bufs) + [block] * len(extra) + [ANY] * len(order),
        out_specs=block,
        out_shape=jax.ShapeDtypeStruct((tok_rows, width), jnp.bfloat16 if last else jnp.float32),
        scratch_shapes=[pltpu.VMEM((used * capacity, width), jnp.bfloat16), pltpu.SemaphoreType.DMA((used,))],
        compiler_params=pltpu.CompilerParams(vmem_limit_bytes=VMEM_LIMIT),
        cost_estimate=pl.CostEstimate(flops=4 * tok_rows * used * capacity * width, bytes_accessed=8 * tok_rows * width, transcendentals=0),
    )(scal, *idx, *probs, *bufs, *extra, *order)


def kept_positions(all_ids, experts, capacity):
    rows = all_ids.shape[1]
    hit = all_ids.transpose(0, 2, 1)[:, :, None, :] == jnp.arange(experts)[:, None]
    hit_bf16 = hit.astype(jnp.bfloat16)
    before = jnp.arange(rows)[:, None] < jnp.arange(rows)[None, :]
    rank = jnp.einsum("sket,tu->skeu", hit_bf16, before.astype(jnp.bfloat16), preferred_element_type=jnp.float32)
    totals = jnp.sum(hit.astype(jnp.int32), axis=-1)
    rank = rank.astype(jnp.int32)
    rank = jnp.stack([rank[:, 0], rank[:, 1] + totals[:, 0, :, None]], axis=1)
    rank = jnp.where(hit & (rank < capacity), rank, -1)
    return jnp.max(rank, axis=1), rank, jnp.minimum(totals[:, 0] + totals[:, 1], capacity)


def solution(mesh):
    token_spec = P(("dp", "ep"), None)
    expert_spec = P("ep", None, None)

    def local_block(hidden, expert_ids, norm_gain, w_router, w_gate, w_up, w_down):
        tok_rows, _ = hidden.shape
        experts = w_router.shape[1]
        local_experts = w_gate.shape[0]
        capacity = (5 * tok_rows + 2 * experts - 1) // (2 * experts)
        me = lax.axis_index("ep")
        core, chip = me % 2, me // 2

        def send(x, pairs):
            return lax.ppermute(x, "ep", pairs)

        swap = [(0, 1), (1, 0), (2, 3), (3, 2)]
        normed = rms_norm(hidden, norm_gain)
        sib = send(normed, swap)
        far_a1 = send(normed, [(0, 3), (2, 1)])

        all_ids = lax.all_gather(expert_ids, "ep", axis=0, tiled=False)
        table, rank, counts = kept_positions(all_ids, experts, capacity)
        mine = lax.dynamic_slice_in_dim(table, me * local_experts, local_experts, axis=1)
        my_counts = lax.dynamic_slice_in_dim(counts, me * local_experts, local_experts, axis=1)

        def pick_shard(x, shard):
            return lax.dynamic_index_in_dim(x, shard, axis=0, keepdims=False)

        other = 1 - chip
        pos_own, cnt_own = pick_shard(mine, me), pick_shard(my_counts, me)
        pos_sib, cnt_sib = pick_shard(mine, 2 * chip + 1 - core), pick_shard(my_counts, 2 * chip + 1 - core)
        pos_a, cnt_a = pick_shard(mine, 2 * other), pick_shard(my_counts, 2 * other)
        pos_b, cnt_b = pick_shard(mine, 2 * other + 1), pick_shard(my_counts, 2 * other + 1)

        def scalars(*xs):
            return jnp.stack([core.astype(jnp.int32)] + [x.astype(jnp.int32) for x in xs])

        weights = (w_gate, w_up, w_down)
        wide = (480, 560, 640)
        narrow = (256, 320)
        order = jnp.zeros((8, 128), jnp.int32)
        (own0, for_sib0), order = ffn_pass(
            (0,), 2, False, wide, capacity, scalars(cnt_own[0], cnt_sib[0]),
            jnp.stack([pos_own[0], pos_sib[0]]), (normed, sib), *weights, order)
        far_a1, normed_late, order = lax.optimization_barrier((far_a1, normed, order))
        far_a0 = send(far_a1, [(3, 2), (1, 0)])
        far_b0 = send(normed_late, [(1, 2), (3, 0)])
        sib_back0 = send(for_sib0, swap)
        (out_a,), order = ffn_pass(
            (0, 1), 1, True, narrow, capacity, scalars(cnt_a[0], cnt_a[1]), pos_a, (far_a0, far_a1), *weights, order)
        far_b0, order = lax.optimization_barrier((far_b0, order))
        far_b1 = send(far_b0, [(2, 3), (0, 1)])
        back_a = [send(out_a, [(0, 2), (2, 0)]), send(out_a, [(1, 2), (3, 0)])]
        (out_b,), order = ffn_pass(
            (0, 1), 1, True, narrow, capacity, scalars(cnt_b[0], cnt_b[1]), pos_b, (far_b0, far_b1), *weights, order)
        back_b = [send(out_b, [(0, 3), (2, 1)]), send(out_b, [(1, 3), (3, 1)])]
        (own1, for_sib1), order = ffn_pass(
            (1,), 2, False, wide, capacity, scalars(cnt_own[1], cnt_sib[1]),
            jnp.stack([pos_own[1], pos_sib[1]]), (normed, sib), *weights, order)
        sib_back1 = send(for_sib1, swap)

        logits = jnp.dot(normed, w_router, preferred_element_type=jnp.float32)
        hit_mask = expert_ids[:, :, None] == jnp.arange(experts)[None, None, :]
        picked = jnp.sum(jnp.where(hit_mask, logits[:, None, :], 0.0), axis=-1)
        probs = jax.nn.softmax(picked, axis=-1)
        probs = [probs[:, 0:1], probs[:, 1:2]]
        my_rank = jnp.max(pick_shard(rank, me), axis=1)
        e0 = expert_ids
        rank_t = jnp.stack([my_rank[0], my_rank[1]], axis=1)
        kept = rank_t >= 0
        owner = e0 // local_experts
        local_no = e0 % local_experts
        near_row = (jnp.where(owner == me, 0, local_experts) + local_no) * capacity + rank_t
        near_row = jnp.where(kept & (owner // 2 == chip), near_row, -1)
        far_row = ((owner % 2) * local_experts + local_no) * capacity + rank_t
        far_row = jnp.where(kept & (owner // 2 != chip), far_row, -1)
        scal = scalars()
        part = combine(scal, [near_row[:, 0:1], near_row[:, 1:2]], probs, [own0, own1, sib_back0, sib_back1], False, [], [])
        return combine(scal, [far_row[:, 0:1], far_row[:, 1:2]], probs, back_a + back_b, True, [hidden, part], [])

    return jax.shard_map(local_block, mesh=mesh,
                         in_specs=(token_spec, token_spec, P(None), P(None, None), expert_spec, expert_spec, expert_spec),
                         out_specs=token_spec, check_vma=False)
```
